32 devices in a mesh: gx: 4 (over z), gy: 8 (over y, x, core).
Axes of the slice: x: 2, y: 2, z: 4, core: 2. Of those that a mesh axis runs over, the one named last changes fastest.
Arguments:
- tokens: bfloat16 [2048, 6144], P('gy', 'gx'), may hold values from -7.5 to 7.5, as said below
- norm_gain: float32 [6144], P('gx'), may hold values from 0.1 to 1.9
- joined_weight: bfloat16 [6144, 43008], P('gx', 'gy'), may hold values from -0.078125 to 0.078125
Outputs:
- projected: bfloat16 [256, 8, 43008], P('gx', None, 'gy')
The draws below stay inside these ranges and needn't reach their ends.
Inputs may be any that keep to these rules, and one draw needn't show every extreme that they name: Every entry of tokens lies between -7.5 and 7.5; each token's features are noise plus an offset of its own plus a slope of its own times a ramp from -1 to 1 over the 6144 features.
All inputs are finite; a program needn't handle non-finite values.
Results may differ from the reference program's by a relative error of at most 0.014.
Values may be sent and summed in bfloat16 or wider, within the bound.
A program may use at most 128 MiB of HBM per device.

```python
import jax
import jax.numpy as jnp
from jax import lax

D = 6144
F = 43008
TOK_DEV = 256
TOKENS = 2048
N_GX = 4
N_GY = 8


def draw_tokens(key, part):
    noise_key = jax.random.fold_in(key, 11)
    offset_key = jax.random.fold_in(key, 12)
    slope_key = jax.random.fold_in(key, 13)
    noise = jnp.clip(jax.random.normal(noise_key, (TOKENS, D), jnp.float32), -4.0, 4.0)
    offset = jnp.clip(0.5 * jax.random.normal(offset_key, (TOKENS, 1), jnp.float32), -2.0, 2.0)
    slope = jax.random.uniform(slope_key, (TOKENS, 1), jnp.float32, -1.5, 1.5)
    ramp = (2.0 * jnp.arange(D, dtype=jnp.float32) + 1.0) / D - 1.0
    values = noise + offset + slope * ramp[None, :]
    return jnp.clip(values, -7.5, 7.5).astype(jnp.bfloat16)


def block_levels(key, shape, pieces, low, largest):
    def one(axis_at, shards_of):
        draws = jax.random.uniform(jax.random.fold_in(jax.random.fold_in(key, 6), axis_at), (shards_of,), jnp.float32, low / len(pieces), largest / len(pieces))
        return jnp.repeat(jnp.exp(draws), shape[axis_at] // shards_of).reshape((-1,) + (1,) * (len(shape) - axis_at - 1))

    level = one(*pieces[0])
    for cut in pieces[1:]:
        level = level * one(*cut)
    return level


def bell_draw(key, extent, spread, bound, shards=(), held_as=jnp.bfloat16):
    values = spread * jax.random.normal(key, extent, jnp.float32)
    if shards:
        values = values * block_levels(key, extent, shards, -0.22, 0.18)
    return jnp.clip(values, -bound, bound).astype(held_as)


def setup_inputs(seed: int = 0) -> dict:
    key_of = jax.random.split(jax.random.key(seed), 4)
    return {
        "tokens": draw_tokens(jax.random.fold_in(key_of[3], 71), 0),
        "norm_gain": jnp.clip(1.0 + 0.18 * jax.random.normal(key_of[1], (D,), jnp.float32), 0.1, 1.9),
        "joined_weight": bell_draw(key_of[2], (D, F), D ** -0.5, 0.078125, ((0, 4), (1, 8))),
    }


epsilon = 1e-06

def reference(tokens, norm_gain, joined_weight):
    values = tokens.astype(jnp.float32)
    mean = lax.optimization_barrier(jnp.sum(values, axis=1, keepdims=True)) / D
    centered = values - mean
    variance = lax.optimization_barrier(jnp.sum(centered * centered, axis=1, keepdims=True)) / D
    normed = (centered * lax.rsqrt(variance + epsilon) * norm_gain).astype(jnp.bfloat16)
    block_width = D // N_GX
    total = jnp.zeros((normed.shape[0], joined_weight.shape[1]), jnp.float32)
    for block in range(N_GX):
        lower = block * block_width
        term = jnp.dot(normed[:, lower:lower + block_width], joined_weight[lower:lower + block_width, :], preferred_element_type=jnp.float32)
        rounded = lax.optimization_barrier(term.astype(jnp.bfloat16))
        total = total + rounded.astype(jnp.float32)
    whole = total.astype(jnp.bfloat16)
    return jnp.transpose(whole.reshape(N_GY, TOK_DEV, whole.shape[1]), (1, 0, 2))
```

```python
import functools

import jax
import jax.numpy as jnp
from jax import lax
from jax.experimental import pallas as pl
from jax.experimental.pallas import tpu as pltpu
from jax.sharding import PartitionSpec as P

MESH = pl.DeviceIdType.MESH
EPSILON = 1e-06
SKEW = 1
STAGES = 4


def partner(y, step, ny):
    out, bit = 0, 1
    while bit < ny:
        out = out + bit * ((y // bit + step // bit) % 2)
        bit *= 2
    return out


def kernel(n, ny, width, tok_ref, gain_ref, w_hbm, out_hbm, w_s, gat, stat, recv, acc, stg, ostg,
           tok_sem, w_sem, stat_send, stat_recv, gat_send, gat_recv, send_sem, recv_sem, out_sem):
    z, y = lax.axis_index("gx"), lax.axis_index("gy")
    tok, depth = tok_ref.shape
    part = tok // n
    columns = w_hbm.shape[1]
    tiles = columns // width
    chunks = ny * tiles
    last_lag = SKEW * (n - 1) + 1
    ring = last_lag + 1
    model = depth * n

    def cols(tile):
        if tiles == 1:
            return slice(None)
        return pl.ds(pl.multiple_of(tile * width, 128), width)

    def w_copy(tile):
        return pltpu.make_async_copy(w_hbm.at[:, cols(tile)], w_s.at[tile], w_sem.at[tile])

    tok_copy = pltpu.make_async_copy(tok_ref, gat.at[0], tok_sem)
    tok_copy.start()
    for tile in range(tiles):
        w_copy(tile).start()

    barrier = pltpu.get_barrier_semaphore()
    for k in range(1, n):
        pl.semaphore_signal(barrier, inc=1, device_id=((z + k) % n, y), device_id_type=MESH)
    for k in range(1, ny):
        pl.semaphore_signal(barrier, inc=1, device_id=(z, partner(y, k, ny)), device_id_type=MESH)

    tok_copy.wait()
    values = gat[0].astype(jnp.float32)
    total = jnp.sum(values, axis=1, keepdims=True)
    off = values - total / depth
    squares = jnp.sum(off * off, axis=1, keepdims=True)
    lane = lax.broadcasted_iota(jnp.int32, (tok, 128), 1)
    packed = jnp.where(lane == 0, total, squares)
    stat[z] = packed.T[:8]

    pl.semaphore_wait(barrier, n - 1 + ny - 1)

    def stat_copy(k):
        return pltpu.make_async_remote_copy(
            src_ref=stat.at[z], dst_ref=stat.at[z], send_sem=stat_send.at[k], recv_sem=stat_recv.at[k],
            device_id=((z + k) % n, y), device_id_type=MESH)

    for k in range(1, n):
        stat_copy(k).start()
    for k in range(1, n):
        source = (z + n - k) % n
        pltpu.make_async_remote_copy(
            src_ref=stat.at[source], dst_ref=stat.at[source], send_sem=stat_send.at[k], recv_sem=stat_recv.at[k],
            device_id=((z + k) % n, y), device_id_type=MESH).wait_recv()
    sums = [stat[k, 0:1, :] for k in range(n)]
    mean = functools.reduce(lambda a, b: a + b, sums) / model
    spread = jnp.zeros_like(mean)
    for k in range(n):
        shift = sums[k] / depth - mean
        spread = spread + stat[k, 1:2, :] + depth * shift * shift
    rstd = lax.rsqrt(spread / model + EPSILON)
    mean_col = jnp.broadcast_to(mean, (128, tok)).T[:, 0:1]
    rstd_col = jnp.broadcast_to(rstd, (128, tok)).T[:, 0:1]
    gat[0] = ((gat[0].astype(jnp.float32) - mean_col) * rstd_col * gain_ref[...]).astype(jnp.bfloat16)

    def gat_copy(k):
        return pltpu.make_async_remote_copy(
            src_ref=gat.at[0], dst_ref=gat.at[k], send_sem=gat_send.at[k], recv_sem=gat_recv.at[k],
            device_id=(z, partner(y, k, ny)), device_id_type=MESH)

    def started():
        for k in range(1, ny):
            gat_copy(k).start()

    def z_copy(stage, index, slot, chunk, to):
        return pltpu.make_async_remote_copy(
            src_ref=stg.at[stage, index], dst_ref=recv.at[slot, chunk], send_sem=send_sem.at[stage, index],
            recv_sem=recv_sem.at[slot, chunk], device_id=(to, y), device_id_type=MESH)

    def arrived(slot, chunk):
        pltpu.make_async_remote_copy(
            src_ref=recv.at[slot, chunk], dst_ref=recv.at[slot, chunk], send_sem=send_sem.at[0, 0],
            recv_sem=recv_sem.at[slot, chunk], device_id=((z + 1) % n, y), device_id_type=MESH).wait_recv()

    def rows(plane):
        return pl.ds(pl.multiple_of(plane * part, part), part)

    def out_copy(chunk):
        token_block = partner(y, chunk // tiles, ny)
        return pltpu.make_async_copy(
            ostg.at[chunk % 2], out_hbm.at[token_block, :, cols(chunk % tiles)], out_sem.at[chunk % 2])

    def forward(chunk, plane, index, out_slot, in_slot, first, to):
        stage = chunk % STAGES

        @pl.when(chunk >= STAGES)
        def _():
            z_copy(stage, index, out_slot, chunk, to).wait_send()

        @pl.when(first)
        def _():
            stg[stage, index] = acc[chunk % ring, rows(plane), :]

        @pl.when(jnp.logical_not(first))
        def _():
            arrived(in_slot, chunk)
            stg[stage, index] = (
                acc[chunk % ring, rows(plane), :].astype(jnp.float32) + recv[in_slot, chunk].astype(jnp.float32)
            ).astype(jnp.bfloat16)

        z_copy(stage, index, out_slot, chunk, to).start()

    started()

    @pl.loop(0, chunks + last_lag)
    def _(it):
        @pl.when(it < chunks)
        def _():
            tile, group = it % tiles, it // tiles

            @pl.when(group == 0)
            def _():
                w_copy(tile).wait()

            @pl.when(jnp.logical_and(group > 0, tile == 0))
            def _():
                gat_copy(group).wait_recv()

            acc[it % ring] = jnp.dot(gat[group], w_s[tile], preferred_element_type=jnp.float32).astype(jnp.bfloat16)

        right = it - SKEW * z

        @pl.when(jnp.logical_and(right >= 0, right < chunks))
        def _():
            for j in reversed(range(n - 1)):
                @pl.when(z + 1 + j < n)
                def _():
                    forward(right, z + 1 + j, j, j, j + 1, z == 0, z + 1)

        left = it - SKEW * (n - 1 - z)

        @pl.when(jnp.logical_and(left >= 0, left < chunks))
        def _():
            for j in reversed(range(n - 1)):
                @pl.when(z - 1 - j >= 0)
                def _():
                    forward(left, z - 1 - j, n - 2 - j, n - j, n - 1 - j, z == n - 1, z - 1)

        own = it - last_lag

        @pl.when(own >= 0)
        def _():
            @pl.when(own >= 2)
            def _():
                out_copy(own - 2).wait()

            mine = acc[own % ring, rows(z), :].astype(jnp.float32)

            @pl.when(z == 0)
            def _():
                arrived(n, own)
                ostg[own % 2] = (mine + recv[n, own].astype(jnp.float32)).astype(jnp.bfloat16)

            @pl.when(z == n - 1)
            def _():
                arrived(0, own)
                ostg[own % 2] = (mine + recv[0, own].astype(jnp.float32)).astype(jnp.bfloat16)

            @pl.when(jnp.logical_and(z > 0, z < n - 1))
            def _():
                arrived(0, own)
                arrived(n, own)
                ostg[own % 2] = (
                    mine + recv[0, own].astype(jnp.float32) + recv[n, own].astype(jnp.float32)
                ).astype(jnp.bfloat16)

            out_copy(own).start()

    for chunk in range(chunks - 2, chunks):
        out_copy(chunk).wait()
    for chunk in range(chunks - STAGES, chunks):
        for index in range(n - 1):
            z_copy(chunk % STAGES, index, 0, chunk, (z + 1) % n).wait_send()
    for k in range(1, n):
        stat_copy(k).wait_send()
    for k in range(1, ny):
        gat_copy(k).wait_send()


def tile_width(columns):
    if columns % 128:
        return columns
    lanes = columns // 128
    return 128 * max(k for k in range(1, 8) if lanes % k == 0)


def solution(mesh):
    n, ny = mesh.shape["gx"], mesh.shape["gy"]

    def body(tokens, norm_gain, joined_weight):
        tok, depth = tokens.shape
        columns = joined_weight.shape[1]
        part, width = tok // n, tile_width(columns)
        tiles = columns // width
        chunks = ny * tiles
        ring = SKEW * (n - 1) + 2
        dma = pltpu.SemaphoreType.DMA
        out = pl.pallas_call(
            functools.partial(kernel, n, ny, width),
            out_shape=jax.ShapeDtypeStruct((ny, part, columns), jnp.bfloat16),
            in_specs=[
                pl.BlockSpec(memory_space=pl.ANY),
                pl.BlockSpec(memory_space=pltpu.VMEM),
                pl.BlockSpec(memory_space=pl.ANY),
            ],
            out_specs=pl.BlockSpec(memory_space=pl.ANY),
            scratch_shapes=[
                pltpu.VMEM((tiles, depth, width), jnp.bfloat16),
                pltpu.VMEM((ny, tok, depth), jnp.bfloat16),
                pltpu.VMEM((n, 8, tok), jnp.float32),
                pltpu.VMEM((n + 1, chunks, part, width), jnp.bfloat16),
                pltpu.VMEM((ring, tok, width), jnp.bfloat16),
                pltpu.VMEM((STAGES, n - 1, part, width), jnp.bfloat16),
                pltpu.VMEM((2, part, width), jnp.bfloat16),
                dma, dma((tiles,)), dma((n,)), dma((n,)), dma((ny,)), dma((ny,)),
                dma((STAGES, n - 1)), dma((n + 1, chunks)), dma((2,)),
            ],
            compiler_params=pltpu.CompilerParams(
                collective_id=0, has_side_effects=True, vmem_limit_bytes=67043328),
        )(tokens, norm_gain.reshape(1, depth), joined_weight)
        return jnp.transpose(out, (1, 0, 2))

    return jax.shard_map(
        body,
        mesh=mesh,
        in_specs=(P("gy", "gx"), P("gx"), P("gx", "gy")),
        out_specs=P("gx", None, "gy"),
        check_vma=False,
    )
```
